32 devices in a mesh: dp: 2 (over x), expert: 4 (over z), seq: 4 (over y, core).
Axes of the slice: x: 2, y: 2, z: 4, core: 2. Of those that a mesh axis runs over, the one named last changes fastest.
Arguments:
- tokens: bfloat16 [4096, 1024], P(('dp', 'expert', 'seq')), parts along dimension 0, may hold values from -6 to 6
- picks: int32 [32, 4, 16], P(('dp', 'expert', 'seq')), parts along dimension 0, may hold values from 0 to 127, as said below
- gates: float32 [32, 4, 16], P(('dp', 'expert', 'seq')), parts along dimension 0, may hold values from 0.1 to 2
- counts: int32 [32, 4], P(('dp', 'expert', 'seq')), parts along dimension 0, may hold values from 1 to 16, as said below
- norm_in: float32 [1024], replicated, may hold values from 0.1 to 1.9
- norm_out: float32 [1024], replicated, may hold values from 0.1 to 1.9
- w_in: bfloat16 [4, 1024, 1408], P('expert'), may hold values from -0.1875 to 0.1875
- w_out: bfloat16 [4, 1408, 1024], P('expert'), may hold values from -0.15625 to 0.15625
- w_key: bfloat16 [1024, 512], replicated, may hold values from -0.1875 to 0.1875
- w_value: bfloat16 [1024, 512], replicated, may hold values from -0.1875 to 0.1875
- queries: bfloat16 [1024, 512], P(('dp', 'expert', 'seq')), parts along dimension 0, may hold values from -300 to 300
- w_proj: bfloat16 [512, 1024], replicated, may hold values from -0.25 to 0.25
Outputs:
- encoded: bfloat16 [4096, 1024], P(('dp', 'expert', 'seq')), parts along dimension 0
- dec_out: bfloat16 [1024, 1024], P(('dp', 'expert', 'seq')), parts along dimension 0
The draws below stay inside these ranges and needn't reach their ends.
There are 2 independent parts, one for each index of `dp`. The reference program is written for one: setup_inputs(seed, part) draws one part's arguments, and reference() takes and returns one part's arrays. A program takes and returns all parts, laid end to end along the dimension named above; an argument that names none is the same for every part. Nothing has to cross between parts.
Inputs may be any that keep to these rules, and one draw needn't show every extreme that they name: `picks`: for each source device and expert, 16 different row numbers of that device's 128 tokens. Slots c < counts are live, the rest are padding; some source device and expert has all 16 slots live.
All inputs are finite; a program needn't handle non-finite values.
Results may differ from the reference program's by a relative error of at most 0.015.
The reference program's roundings to bfloat16 on the way count: a program that leaves them out, or rounds other values in their place, can miss the bound.
Values may be sent and summed in bfloat16 or wider, within the bound.
A program may use at most 64 MiB of HBM per device.

```python
import math
import jax
import jax.numpy as jnp
from jax import lax

D = 1024
FF = 1408
HEADS = 8
TOK_DEV = 128
DEC_DEV = 32
EXPERTS = 4
CAP = 16
SOURCES = 16
TOKENS = 2048
DEC_TOKENS = 512
HQ = 512
N_EXPERT = 4
N_SEQ = 4


def draw_picks(key, part):
    subkeys = jax.random.split(jax.random.fold_in(key, 11), SOURCES * EXPERTS)

    def choose(subkey):
        return jax.random.permutation(subkey, TOK_DEV)[:CAP]
    chosen = jax.vmap(choose)(subkeys)
    return chosen.reshape(SOURCES, EXPERTS, CAP).astype(jnp.int32)


def draw_counts(key, part):
    first, second = jax.random.split(jax.random.fold_in(key, 23))
    drawn = jax.random.randint(first, (SOURCES * EXPERTS,), 1, CAP + 1, dtype=jnp.int32)
    position = jax.random.randint(second, (), 0, SOURCES * EXPERTS, dtype=jnp.int32)
    drawn = drawn.at[position].set(CAP)
    return drawn.reshape(SOURCES, EXPERTS).astype(jnp.int32)


def draw_queries(key, part):
    first = jax.random.fold_in(jax.random.fold_in(key, 37), 0)
    base = jnp.clip(jax.random.normal(first, (DEC_TOKENS, HQ), jnp.float32), -6.0, 6.0)
    return base.astype(jnp.bfloat16)


def levels(own_key, dims, pieces, low, largest):
    level, own = 1.0, jax.random.fold_in(own_key, 6)
    for dim, blocks in pieces:
        heights = jnp.exp(jax.random.uniform(jax.random.fold_in(own, dim), (blocks,), jnp.float32, low / len(pieces), largest / len(pieces)))
        level = level * jnp.repeat(heights, dims[dim] // blocks).reshape([-1 if axis == dim else 1 for axis in range(len(dims))])
    return level


def scatter_about(own_key, dims, scale, bound, shards=(), kind=jnp.bfloat16):
    array = jax.random.normal(own_key, dims, jnp.float32) * scale
    if len(shards) > 0:
        array = levels(own_key, dims, shards, -0.22, 0.18) * array
    return jnp.clip(array, min=-bound, max=bound).astype(kind)


def setup_inputs(seed: int = 0, part: int = 0) -> dict:
    key_of = jax.random.split(jax.random.key(seed), 13)
    part_splits = jax.random.split(jax.random.fold_in(key_of[12], part), 13)
    return {
        "tokens": scatter_about(part_splits[0], (TOKENS, D), 1.0, 6.0, ((0, 16),)),
        "picks": draw_picks(jax.random.fold_in(jax.random.fold_in(key_of[12], part), 71), part),
        "gates": jnp.clip(jnp.exp(math.log(2.0) - 2.9957323 * jax.random.uniform(part_splits[2], (SOURCES, EXPERTS, CAP), jnp.float32) ** levels(part_splits[2], (SOURCES, EXPERTS, CAP), ((0, 16),), -0.2, 0.2)), 0.1, 2.0),
        "counts": draw_counts(jax.random.fold_in(jax.random.fold_in(key_of[12], part), 71), part),
        "norm_in": jnp.clip(1.0 + 0.18 * jax.random.normal(key_of[4], (D,), jnp.float32), 0.1, 1.9),
        "norm_out": jnp.clip(1.0 + 0.18 * jax.random.normal(key_of[5], (D,), jnp.float32), 0.1, 1.9),
        "w_in": scatter_about(key_of[6], (EXPERTS, D, FF), D ** -0.5, 0.1875, ((0, 4),)),
        "w_out": scatter_about(key_of[7], (EXPERTS, FF, D), FF ** -0.5, 0.15625, ((0, 4),)),
        "w_key": scatter_about(key_of[8], (D, HQ), D ** -0.5, 0.1875),
        "w_value": scatter_about(key_of[9], (D, HQ), D ** -0.5, 0.1875),
        "queries": draw_queries(jax.random.fold_in(jax.random.fold_in(key_of[12], part), 71), part),
        "w_proj": scatter_about(key_of[11], (HQ, D), HQ ** -0.5, 0.25),
    }


EPSILON = 1e-06

def rms_norm(values, gain):
    mean_square = lax.optimization_barrier(jnp.mean(values * values, axis=-1, keepdims=True))
    return values * lax.rsqrt(mean_square + EPSILON) * gain

def reference(tokens, picks, gates, counts, norm_in, norm_out, w_in, w_out, w_key, w_value, queries, w_proj):
    model_width = tokens.shape[1]
    plain = tokens.astype(jnp.float32)
    normed = rms_norm(plain, norm_in.astype(jnp.float32)).astype(jnp.bfloat16)
    offsets = jnp.arange(SOURCES, dtype=jnp.int32) * TOK_DEV
    row_index = (picks + offsets[:, None, None]).astype(jnp.int32)

    def expert_apply(expert):
        chosen = jnp.take(normed, row_index[:, expert, :].reshape(-1), axis=0)
        hidden = jax.nn.gelu(jnp.dot(chosen, w_in[expert], preferred_element_type=jnp.float32), approximate=True).astype(jnp.bfloat16)
        return jnp.dot(hidden, w_out[expert], preferred_element_type=jnp.float32).astype(jnp.bfloat16)
    outputs = lax.map(expert_apply, jnp.arange(EXPERTS, dtype=jnp.int32))
    ordered = outputs.reshape(EXPERTS, SOURCES, CAP, model_width).transpose(1, 0, 2, 3)
    live = (jnp.arange(CAP, dtype=jnp.int32)[None, None, :] < counts[:, :, None]).astype(jnp.float32)
    slot_weight = gates.astype(jnp.float32) * live
    terms = ordered.astype(jnp.float32) * slot_weight[..., None]
    expert_sum = jnp.zeros((TOKENS, model_width), jnp.float32).at[row_index.reshape(-1)].add(terms.reshape(-1, model_width))
    mixed = plain + expert_sum
    encoded = rms_norm(mixed, norm_out.astype(jnp.float32)).astype(jnp.bfloat16)
    key_proj = jnp.dot(encoded, w_key, preferred_element_type=jnp.float32).astype(jnp.bfloat16)
    value_proj = jnp.dot(encoded, w_value, preferred_element_type=jnp.float32).astype(jnp.bfloat16)
    head_size = queries.shape[1] // HEADS
    seq_length = N_SEQ * TOK_DEV
    key_heads = key_proj.reshape(N_EXPERT, seq_length, HEADS, head_size)
    value_heads = value_proj.reshape(N_EXPERT, seq_length, HEADS, head_size)
    query_heads = queries.reshape(N_EXPERT, N_SEQ * DEC_DEV, HEADS, head_size)

    def attend(inputs):
        query_block, key_block, value_block = inputs
        scores = jnp.einsum('qhd,khd->qhk', query_block.astype(jnp.float32), key_block.astype(jnp.float32)) * head_size ** (-0.5)
        row_max = lax.optimization_barrier(jnp.max(scores, axis=-1, keepdims=True))
        weights = jnp.exp(scores - row_max)
        row_total = lax.optimization_barrier(jnp.sum(weights, axis=-1))
        rounded = lax.optimization_barrier(weights.astype(jnp.bfloat16)).astype(jnp.float32)
        context = jnp.einsum('qhk,khd->qhd', rounded, value_block.astype(jnp.float32)) / row_total[..., None]
        return context.astype(jnp.bfloat16)
    contexts = lax.map(attend, (query_heads, key_heads, value_heads))
    context = contexts.reshape(DEC_TOKENS, HEADS * head_size)
    dec_out = jnp.dot(context, w_proj, preferred_element_type=jnp.float32).astype(jnp.bfloat16)
    return (encoded, dec_out)
```

```python
import functools

import jax
import jax.numpy as jnp
from jax import lax
from jax.experimental import pallas as pl
from jax.experimental.pallas import tpu as pltpu
from jax.sharding import PartitionSpec as P

HEADS = 8
EPSILON = 1e-06
MESH = pl.DeviceIdType.MESH
F32 = jnp.float32
BF16 = jnp.bfloat16


def rms_norm(values, gain):
    mean_square = jnp.mean(values * values, axis=-1, keepdims=True)
    return values * lax.rsqrt(mean_square + EPSILON) * gain


def gelu(v):
    return 0.5 * v * (1.0 + jnp.tanh(0.7978845608028654 * (v + 0.044715 * v * v * v)))


def kernel(
    n_e,
    n_s,
    tokens_h,
    picks_h,
    gates_h,
    counts_h,
    norm_in_h,
    norm_out_h,
    w_in_h,
    w_out_h,
    w_key_h,
    w_value_h,
    queries_h,
    w_proj_h,
    encoded_h,
    dec_h,
    tokens_v,
    picks_v,
    gates_v,
    counts_v,
    norm_in_v,
    norm_out_v,
    w_in_v,
    w_out_v,
    w_key_v,
    w_value_v,
    q_v,
    w_proj_v,
    send_a,
    recv_a,
    send_b,
    recv_b,
    enc_v,
    part_v,
    stat_v,
    part_r,
    stat_r,
    dec_v,
    load_sem,
    store_sem,
    a_send,
    a_recv,
    b_send,
    b_recv,
    q_send,
    q_recv,
    p_send,
    p_recv,
    s_send,
    s_recv,
):
    me_e = lax.axis_index("expert")
    me_s = lax.axis_index("seq")
    rows, width = tokens_v.shape
    slots = send_a.shape[1]
    dec_rows = q_v.shape[1]
    q_width = q_v.shape[2]
    head = q_width // HEADS

    loads = {}
    for i, (name, src, dst) in enumerate(
        (
            ("tokens", tokens_h, tokens_v),
            ("norm_in", norm_in_h, norm_in_v),
            ("picks", picks_h, picks_v),
            ("queries", queries_h, q_v.at[me_s]),
            ("w_in", w_in_h.at[0], w_in_v),
            ("w_out", w_out_h.at[0], w_out_v),
            ("gates", gates_h, gates_v),
            ("counts", counts_h, counts_v),
            ("norm_out", norm_out_h, norm_out_v),
            ("w_key", w_key_h, w_key_v),
            ("w_value", w_value_h, w_value_v),
            ("w_proj", w_proj_h, w_proj_v),
        )
    ):
        loads[name] = pltpu.make_async_copy(src, dst, load_sem.at[i])
        loads[name].start()

    barrier = pltpu.get_barrier_semaphore()
    for d in range(1, n_e):
        pl.semaphore_signal(
            barrier, inc=1, device_id={"expert": lax.rem(me_e + d, n_e)}, device_id_type=MESH
        )
    for d in range(1, n_s):
        pl.semaphore_signal(
            barrier, inc=1, device_id={"seq": lax.rem(me_s + d, n_s)}, device_id_type=MESH
        )

    loads["tokens"].wait()
    loads["norm_in"].wait()
    loads["picks"].wait()
    normed = rms_norm(tokens_v[...].astype(F32), norm_in_v[...]).astype(BF16)
    pick_row = jnp.concatenate([picks_v[0, j : j + 1, :] for j in range(n_e)], axis=1)
    position = lax.broadcasted_iota(jnp.int32, (rows, n_e * slots), 0)
    chosen = jnp.where(position == pick_row, 1.0, 0.0).astype(BF16)
    outgoing = lax.dot_general(
        chosen, normed, (((0,), (0,)), ((), ())), preferred_element_type=F32
    ).astype(BF16)
    send_a[...] = outgoing.reshape(n_e, slots, width)
    pl.semaphore_wait(barrier, n_e - 1 + n_s - 1)

    a_copies = []
    for d in range(1, n_e):
        to = lax.rem(me_e + d, n_e)
        copy = pltpu.make_async_remote_copy(
            src_ref=send_a.at[to],
            dst_ref=recv_a.at[d],
            send_sem=a_send.at[d],
            recv_sem=a_recv.at[d],
            device_id={"expert": to},
            device_id_type=MESH,
        )
        copy.start()
        a_copies.append(copy)
    loads["queries"].wait()
    q_copies = []
    for d in range(1, n_s):
        copy = pltpu.make_async_remote_copy(
            src_ref=q_v.at[me_s],
            dst_ref=q_v.at[me_s],
            send_sem=q_send.at[d],
            recv_sem=q_recv.at[d],
            device_id={"seq": lax.rem(me_s + d, n_s)},
            device_id_type=MESH,
        )
        copy.start()
        q_copies.append(copy)
    recv_a[0] = send_a[me_e]

    loads["gates"].wait()
    loads["counts"].wait()
    slot = lax.broadcasted_iota(jnp.int32, (1, slots), 1)
    gate_row = jnp.concatenate(
        [
            jnp.where(slot < counts_v[0:1, j : j + 1], gates_v[0, j : j + 1, :], 0.0)
            for j in range(n_e)
        ],
        axis=1,
    )
    high = gate_row.astype(BF16).astype(F32)
    middle = (gate_row - high).astype(BF16).astype(F32)
    low = gate_row - high - middle
    gate_three = jnp.concatenate([high, middle, low], axis=1)
    pick_three = jnp.concatenate([pick_row] * 3, axis=1)
    position_three = lax.broadcasted_iota(jnp.int32, (rows, 3 * n_e * slots), 0)
    combine = jnp.where(position_three == pick_three, gate_three, 0.0).astype(BF16)

    loads["w_in"].wait()
    for copy in a_copies:
        copy.wait_recv()
    flat = recv_a[...].reshape(n_e * slots, width)
    hidden = gelu(jnp.dot(flat, w_in_v[...], preferred_element_type=F32)).astype(BF16)
    loads["w_out"].wait()
    result = jnp.dot(hidden, w_out_v[...], preferred_element_type=F32).astype(BF16)
    send_b[...] = result.reshape(n_e, slots, width)
    b_copies = []
    for d in range(1, n_e):
        copy = pltpu.make_async_remote_copy(
            src_ref=send_b.at[d],
            dst_ref=recv_b.at[me_e],
            send_sem=b_send.at[d],
            recv_sem=b_recv.at[d],
            device_id={"expert": lax.rem(me_e + n_e - d, n_e)},
            device_id_type=MESH,
        )
        copy.start()
        b_copies.append(copy)
    recv_b[me_e] = send_b[0]

    loads["norm_out"].wait()
    loads["w_key"].wait()
    loads["w_value"].wait()
    for d in range(1, n_e):
        pltpu.make_async_remote_copy(
            src_ref=send_b.at[d],
            dst_ref=recv_b.at[lax.rem(me_e + d, n_e)],
            send_sem=b_send.at[d],
            recv_sem=b_recv.at[d],
            device_id={"expert": lax.rem(me_e + n_e - d, n_e)},
            device_id_type=MESH,
        ).wait_recv()
    returned = recv_b[...].reshape(n_e * slots, width)
    expert_sum = jnp.dot(
        combine, jnp.concatenate([returned] * 3, axis=0), preferred_element_type=F32
    )
    mixed = tokens_v[...].astype(F32) + expert_sum
    encoded = rms_norm(mixed, norm_out_v[...]).astype(BF16)
    enc_v[...] = encoded
    enc_store = pltpu.make_async_copy(enc_v, encoded_h, store_sem.at[0])
    enc_store.start()
    keys = jnp.dot(encoded, w_key_v[...], preferred_element_type=F32).astype(BF16)
    values = jnp.dot(encoded, w_value_v[...], preferred_element_type=F32).astype(BF16)

    for d in range(1, n_s):
        pltpu.make_async_remote_copy(
            src_ref=q_v.at[me_s],
            dst_ref=q_v.at[lax.rem(me_s + n_s - d, n_s)],
            send_sem=q_send.at[d],
            recv_sem=q_recv.at[d],
            device_id={"seq": lax.rem(me_s + d, n_s)},
            device_id_type=MESH,
        ).wait_recv()
    all_rows = n_s * dec_rows
    queries = q_v[...].reshape(all_rows, q_width)
    slab = min(256, q_width)
    group = slab // head
    lane_head = lax.broadcasted_iota(jnp.int32, (1, slab), 1) // head
    stat_lane = lax.broadcasted_iota(jnp.int32, (1, stat_v.shape[2]), 1)
    stats = jnp.zeros((all_rows, stat_v.shape[2]), F32)
    for g in range(q_width // slab):
        cols = slice(g * slab, (g + 1) * slab)
        stacked = jnp.concatenate(
            [
                queries[:, cols] * jnp.where(lane_head == h, 1.0, 0.0).astype(BF16)
                for h in range(group)
            ],
            axis=0,
        )
        scores = lax.dot_general(
            stacked, keys[:, cols], (((1,), (1,)), ((), ())), preferred_element_type=F32
        ) * (head**-0.5)
        row_max = jnp.max(scores, axis=1, keepdims=True)
        weights = jnp.exp(scores - row_max)
        row_total = jnp.sum(weights, axis=1, keepdims=True)
        product = jnp.dot(weights.astype(BF16), values[:, cols], preferred_element_type=F32)
        joined = product[:all_rows]
        for h in range(group):
            span = slice(h * all_rows, (h + 1) * all_rows)
            if h:
                joined = jnp.where(lane_head == h, product[span], joined)
            at = g * group + h
            stats = jnp.where(stat_lane == at, row_max[span], stats)
            stats = jnp.where(stat_lane == HEADS + at, row_total[span], stats)
        part_v[:, :, cols] = joined.astype(BF16).reshape(n_s, dec_rows, slab)
    stat_v[...] = stats.reshape(n_s, dec_rows, stat_v.shape[2])

    p_copies = []
    for d in range(1, n_s):
        to = lax.rem(me_s + d, n_s)
        for src, dst, ss, rs in (
            (stat_v, stat_r, s_send, s_recv),
            (part_v, part_r, p_send, p_recv),
        ):
            copy = pltpu.make_async_remote_copy(
                src_ref=src.at[to],
                dst_ref=dst.at[d],
                send_sem=ss.at[d],
                recv_sem=rs.at[d],
                device_id={"seq": to},
                device_id_type=MESH,
            )
            copy.start()
            p_copies.append(copy)
    loads["w_proj"].wait()
    for copy in p_copies:
        copy.wait_recv()
    part = [part_v[me_s].astype(F32)] + [part_r[d].astype(F32) for d in range(1, n_s)]
    stat = [stat_v[me_s]] + [stat_r[d] for d in range(1, n_s)]
    top = functools.reduce(jnp.maximum, stat)
    factor = [jnp.exp(s - top)[:, :HEADS] for s in stat]
    total = sum(f * s[:, HEADS : 2 * HEADS] for f, s in zip(factor, stat))
    lane = lax.broadcasted_iota(jnp.int32, (1, q_width), 1) // head
    summed = jnp.zeros((dec_rows, q_width), F32)
    for f, p in zip(factor, part):
        scale = f / total
        spread = jnp.zeros((dec_rows, q_width), F32)
        for h in range(HEADS):
            spread = jnp.where(lane == h, scale[:, h : h + 1], spread)
        summed = summed + spread * p
    dec_v[...] = jnp.dot(
        summed.astype(BF16), w_proj_v[...], preferred_element_type=F32
    ).astype(BF16)
    dec_store = pltpu.make_async_copy(dec_v, dec_h, store_sem.at[1])
    dec_store.start()
    for copy in a_copies + b_copies + q_copies + p_copies:
        copy.wait_send()
    enc_store.wait()
    dec_store.wait()


def local(
    n_e,
    n_s,
    tokens,
    picks,
    gates,
    counts,
    norm_in,
    norm_out,
    w_in,
    w_out,
    w_key,
    w_value,
    queries,
    w_proj,
):
    rows, width = tokens.shape
    slots = picks.shape[2]
    hidden = w_in.shape[2]
    dec_rows, q_width = queries.shape
    lanes = max(128, 2 * HEADS)
    anywhere = pl.BlockSpec(memory_space=pl.ANY)
    dma = pltpu.SemaphoreType.DMA
    return pl.pallas_call(
        functools.partial(kernel, n_e, n_s),
        out_shape=(
            jax.ShapeDtypeStruct((rows, width), BF16),
            jax.ShapeDtypeStruct((dec_rows, width), BF16),
        ),
        in_specs=[anywhere] * 12,
        out_specs=(anywhere, anywhere),
        scratch_shapes=[
            pltpu.VMEM((rows, width), BF16),
            pltpu.VMEM(picks.shape, jnp.int32),
            pltpu.VMEM(gates.shape, F32),
            pltpu.VMEM(counts.shape, jnp.int32),
            pltpu.VMEM((1, width), F32),
            pltpu.VMEM((1, width), F32),
            pltpu.VMEM((width, hidden), BF16),
            pltpu.VMEM((hidden, width), BF16),
            pltpu.VMEM((width, q_width), BF16),
            pltpu.VMEM((width, q_width), BF16),
            pltpu.VMEM((n_s, dec_rows, q_width), BF16),
            pltpu.VMEM((q_width, width), BF16),
            pltpu.VMEM((n_e, slots, width), BF16),
            pltpu.VMEM((n_e, slots, width), BF16),
            pltpu.VMEM((n_e, slots, width), BF16),
            pltpu.VMEM((n_e, slots, width), BF16),
            pltpu.VMEM((rows, width), BF16),
            pltpu.VMEM((n_s, dec_rows, q_width), BF16),
            pltpu.VMEM((n_s, dec_rows, lanes), F32),
            pltpu.VMEM((n_s, dec_rows, q_width), BF16),
            pltpu.VMEM((n_s, dec_rows, lanes), F32),
            pltpu.VMEM((dec_rows, width), BF16),
            dma((12,)),
            dma((2,)),
            dma((n_e,)),
            dma((n_e,)),
            dma((n_e,)),
            dma((n_e,)),
            dma((n_s,)),
            dma((n_s,)),
            dma((n_s,)),
            dma((n_s,)),
            dma((n_s,)),
            dma((n_s,)),
        ],
        compiler_params=pltpu.CompilerParams(collective_id=0, has_side_effects=True),
    )(
        tokens,
        picks,
        gates,
        counts,
        norm_in.reshape(1, -1),
        norm_out.reshape(1, -1),
        w_in,
        w_out,
        w_key,
        w_value,
        queries,
        w_proj,
    )


def solution(mesh):
    in_specs = (
        P(("dp", "expert", "seq"), None),
        P(("dp", "expert", "seq"), None, None),
        P(("dp", "expert", "seq"), None, None),
        P(("dp", "expert", "seq"), None),
        P(),
        P(),
        P("expert", None, None),
        P("expert", None, None),
        P(),
        P(),
        P(("dp", "expert", "seq"), None),
        P(),
    )
    out_specs = (P(("dp", "expert", "seq"), None), P(("dp", "expert", "seq"), None))
    body = functools.partial(local, mesh.shape["expert"], mesh.shape["seq"])
    return jax.shard_map(body, mesh=mesh, in_specs=in_specs, out_specs=out_specs, check_vma=False)
```

```python
import functools

import jax
import jax.numpy as jnp
from jax import lax
from jax.experimental import pallas as pl
from jax.experimental.pallas import tpu as pltpu
from jax.sharding import PartitionSpec as P

HEADS = 8
EPSILON = 1e-06
VMEM_BYTES = 67043328
MESH = pl.DeviceIdType.MESH
F32 = jnp.float32
BF16 = jnp.bfloat16


def rms_norm(values, gain):
    mean_square = jnp.mean(values * values, axis=-1, keepdims=True)
    return values * lax.rsqrt(mean_square + EPSILON) * gain


def gelu(v):
    return 0.5 * v * (1.0 + jnp.tanh(0.7978845608028654 * (v + 0.044715 * v * v * v)))


def kernel(
    n_e,
    n_s,
    tokens_h,
    picks_h,
    gates_h,
    counts_h,
    norm_in_h,
    norm_out_h,
    w_in_h,
    w_out_h,
    w_key_h,
    w_value_h,
    queries_h,
    w_proj_h,
    enc_v,
    part_r,
    stat_r,
    w_proj_v,
    tokens_v,
    picks_v,
    gates_v,
    counts_v,
    norm_in_v,
    norm_out_v,
    w_in_v,
    w_out_v,
    w_key_v,
    w_value_v,
    q_v,
    send_a,
    recv_a,
    send_b,
    recv_b,
    part_v,
    stat_v,
    load_sem,
    a_send,
    a_recv,
    b_send,
    b_recv,
    q_send,
    q_recv,
    p_send,
    p_recv,
    s_send,
    s_recv,
):
    me_e = lax.axis_index("expert")
    me_s = lax.axis_index("seq")
    rows, width = tokens_v.shape
    slots = send_a.shape[1]
    dec_rows = q_v.shape[1]
    q_width = q_v.shape[2]
    head = q_width // HEADS

    loads = {}
    for i, (name, src, dst) in enumerate(
        (
            ("tokens", tokens_h, tokens_v),
            ("norm_in", norm_in_h, norm_in_v),
            ("picks", picks_h, picks_v),
            ("queries", queries_h, q_v.at[me_s]),
            ("w_in", w_in_h.at[0], w_in_v),
            ("w_out", w_out_h.at[0], w_out_v),
            ("gates", gates_h, gates_v),
            ("counts", counts_h, counts_v),
            ("norm_out", norm_out_h, norm_out_v),
            ("w_key", w_key_h, w_key_v),
            ("w_value", w_value_h, w_value_v),
            ("w_proj", w_proj_h, w_proj_v),
        )
    ):
        loads[name] = pltpu.make_async_copy(src, dst, load_sem.at[i])
        loads[name].start()

    barrier = pltpu.get_barrier_semaphore()
    for d in range(1, n_e):
        pl.semaphore_signal(
            barrier, inc=1, device_id={"expert": lax.rem(me_e + d, n_e)}, device_id_type=MESH
        )
    for d in range(1, n_s):
        pl.semaphore_signal(
            barrier, inc=1, device_id={"seq": lax.rem(me_s + d, n_s)}, device_id_type=MESH
        )

    loads["tokens"].wait()
    loads["norm_in"].wait()
    loads["picks"].wait()
    normed = rms_norm(tokens_v[...].astype(F32), norm_in_v[...]).astype(BF16)
    pick_row = jnp.concatenate([picks_v[0, j : j + 1, :] for j in range(n_e)], axis=1)
    position = lax.broadcasted_iota(jnp.int32, (rows, n_e * slots), 0)
    chosen = jnp.where(position == pick_row, 1.0, 0.0).astype(BF16)
    outgoing = lax.dot_general(
        chosen, normed, (((0,), (0,)), ((), ())), preferred_element_type=F32
    ).astype(BF16)
    send_a[...] = outgoing.reshape(n_e, slots, width)
    pl.semaphore_wait(barrier, n_e - 1 + n_s - 1)

    a_copies = []
    for d in range(1, n_e):
        to = lax.rem(me_e + d, n_e)
        copy = pltpu.make_async_remote_copy(
            src_ref=send_a.at[to],
            dst_ref=recv_a.at[d],
            send_sem=a_send.at[d],
            recv_sem=a_recv.at[d],
            device_id={"expert": to},
            device_id_type=MESH,
        )
        copy.start()
        a_copies.append(copy)
    loads["queries"].wait()
    q_copies = []
    for d in range(1, n_s):
        copy = pltpu.make_async_remote_copy(
            src_ref=q_v.at[me_s],
            dst_ref=q_v.at[me_s],
            send_sem=q_send.at[d],
            recv_sem=q_recv.at[d],
            device_id={"seq": lax.rem(me_s + d, n_s)},
            device_id_type=MESH,
        )
        copy.start()
        q_copies.append(copy)
    recv_a[0] = send_a[me_e]

    loads["gates"].wait()
    loads["counts"].wait()
    slot = lax.broadcasted_iota(jnp.int32, (1, slots), 1)
    gate_row = jnp.concatenate(
        [
            jnp.where(slot < counts_v[0:1, j : j + 1], gates_v[0, j : j + 1, :], 0.0)
            for j in range(n_e)
        ],
        axis=1,
    )
    high = gate_row.astype(BF16).astype(F32)
    middle = (gate_row - high).astype(BF16).astype(F32)
    low = gate_row - high - middle
    gate_three = jnp.concatenate([high, middle, low], axis=1)
    pick_three = jnp.concatenate([pick_row] * 3, axis=1)
    position_three = lax.broadcasted_iota(jnp.int32, (rows, 3 * n_e * slots), 0)
    combine = jnp.where(position_three == pick_three, gate_three, 0.0).astype(BF16)

    loads["w_in"].wait()
    for copy in a_copies:
        copy.wait_recv()
    flat = recv_a[...].reshape(n_e * slots, width)
    hidden = gelu(jnp.dot(flat, w_in_v[...], preferred_element_type=F32)).astype(BF16)
    loads["w_out"].wait()
    result = jnp.dot(hidden, w_out_v[...], preferred_element_type=F32).astype(BF16)
    send_b[...] = result.reshape(n_e, slots, width)
    b_copies = []
    for d in range(1, n_e):
        copy = pltpu.make_async_remote_copy(
            src_ref=send_b.at[d],
            dst_ref=recv_b.at[me_e],
            send_sem=b_send.at[d],
            recv_sem=b_recv.at[d],
            device_id={"expert": lax.rem(me_e + n_e - d, n_e)},
            device_id_type=MESH,
        )
        copy.start()
        b_copies.append(copy)
    recv_b[me_e] = send_b[0]

    loads["norm_out"].wait()
    loads["w_key"].wait()
    loads["w_value"].wait()
    for d in range(1, n_e):
        pltpu.make_async_remote_copy(
            src_ref=send_b.at[d],
            dst_ref=recv_b.at[lax.rem(me_e + d, n_e)],
            send_sem=b_send.at[d],
            recv_sem=b_recv.at[d],
            device_id={"expert": lax.rem(me_e + n_e - d, n_e)},
            device_id_type=MESH,
        ).wait_recv()
    returned = recv_b[...].reshape(n_e * slots, width)
    expert_sum = jnp.dot(
        combine, jnp.concatenate([returned] * 3, axis=0), preferred_element_type=F32
    )
    mixed = tokens_v[...].astype(F32) + expert_sum
    encoded = rms_norm(mixed, norm_out_v[...]).astype(BF16)
    enc_v[...] = encoded
    keys = jnp.dot(encoded, w_key_v[...], preferred_element_type=F32).astype(BF16)
    values = jnp.dot(encoded, w_value_v[...], preferred_element_type=F32).astype(BF16)

    for d in range(1, n_s):
        pltpu.make_async_remote_copy(
            src_ref=q_v.at[me_s],
            dst_ref=q_v.at[lax.rem(me_s + n_s - d, n_s)],
            send_sem=q_send.at[d],
            recv_sem=q_recv.at[d],
            device_id={"seq": lax.rem(me_s + d, n_s)},
            device_id_type=MESH,
        ).wait_recv()
    all_rows = n_s * dec_rows
    queries = q_v[...].reshape(all_rows, q_width)
    slab = min(256, q_width)
    group = slab // head
    lane_head = lax.broadcasted_iota(jnp.int32, (1, slab), 1) // head
    stat_lane = lax.broadcasted_iota(jnp.int32, (1, stat_v.shape[2]), 1)
    stats = jnp.zeros((all_rows, stat_v.shape[2]), F32)
    for g in range(q_width // slab):
        cols = slice(g * slab, (g + 1) * slab)
        stacked = jnp.concatenate(
            [
                queries[:, cols] * jnp.where(lane_head == h, 1.0, 0.0).astype(BF16)
                for h in range(group)
            ],
            axis=0,
        )
        scores = lax.dot_general(
            stacked, keys[:, cols], (((1,), (1,)), ((), ())), preferred_element_type=F32
        ) * (head**-0.5)
        row_max = jnp.max(scores, axis=1, keepdims=True)
        weights = jnp.exp(scores - row_max)
        row_total = jnp.sum(weights, axis=1, keepdims=True)
        product = jnp.dot(weights.astype(BF16), values[:, cols], preferred_element_type=F32)
        joined = product[:all_rows]
        for h in range(group):
            span = slice(h * all_rows, (h + 1) * all_rows)
            if h:
                joined = jnp.where(lane_head == h, product[span], joined)
            at = g * group + h
            stats = jnp.where(stat_lane == at, row_max[span], stats)
            stats = jnp.where(stat_lane == HEADS + at, row_total[span], stats)
        part_v[:, :, cols] = joined.astype(BF16).reshape(n_s, dec_rows, slab)
    stat_v[...] = stats.reshape(n_s, dec_rows, stat_v.shape[2])

    part_r[0] = part_v[me_s]
    stat_r[0] = stat_v[me_s]
    p_copies = []
    for d in range(1, n_s):
        to = lax.rem(me_s + d, n_s)
        for src, dst, ss, rs in (
            (stat_v, stat_r, s_send, s_recv),
            (part_v, part_r, p_send, p_recv),
        ):
            copy = pltpu.make_async_remote_copy(
                src_ref=src.at[to],
                dst_ref=dst.at[d],
                send_sem=ss.at[d],
                recv_sem=rs.at[d],
                device_id={"seq": to},
                device_id_type=MESH,
            )
            copy.start()
            p_copies.append(copy)
    for copy in p_copies:
        copy.wait_recv()
    for copy in a_copies + b_copies + q_copies + p_copies:
        copy.wait_send()
    loads["w_proj"].wait()


def finish(
    enc_v, part_v, stat_v, w_proj_v, encoded_h, dec_h, dec_v, store_sem
):
    enc_store = pltpu.make_async_copy(enc_v, encoded_h, store_sem.at[0])
    enc_store.start()
    n_s, dec_rows, q_width = part_v.shape
    head = q_width // HEADS
    part = [part_v[d].astype(F32) for d in range(n_s)]
    stat = [stat_v[d] for d in range(n_s)]
    top = functools.reduce(jnp.maximum, stat)
    factor = [jnp.exp(s - top)[:, :HEADS] for s in stat]
    total = sum(f * s[:, HEADS : 2 * HEADS] for f, s in zip(factor, stat))
    lane = lax.broadcasted_iota(jnp.int32, (1, q_width), 1) // head
    summed = jnp.zeros((dec_rows, q_width), F32)
    for f, p in zip(factor, part):
        scale = f / total
        spread = jnp.zeros((dec_rows, q_width), F32)
        for h in range(HEADS):
            spread = jnp.where(lane == h, scale[:, h : h + 1], spread)
        summed = summed + spread * p
    dec_v[...] = jnp.dot(
        summed.astype(BF16), w_proj_v[...], preferred_element_type=F32
    ).astype(BF16)
    dec_store = pltpu.make_async_copy(dec_v, dec_h, store_sem.at[1])
    dec_store.start()
    enc_store.wait()
    dec_store.wait()


def local(
    n_e,
    n_s,
    tokens,
    picks,
    gates,
    counts,
    norm_in,
    norm_out,
    w_in,
    w_out,
    w_key,
    w_value,
    queries,
    w_proj,
):
    rows, width = tokens.shape
    slots = picks.shape[2]
    hidden = w_in.shape[2]
    dec_rows, q_width = queries.shape
    lanes = max(128, 2 * HEADS)
    anywhere = pl.BlockSpec(memory_space=pl.ANY)
    dma = pltpu.SemaphoreType.DMA
    vmem = pl.BlockSpec(memory_space=pltpu.VMEM)
    room = 2 * (rows * width + n_s * dec_rows * (q_width + 2 * lanes) + q_width * width)
    encoded, part, stat, w_proj_near = pl.pallas_call(
        functools.partial(kernel, n_e, n_s),
        out_shape=(
            pltpu.VMEM((rows, width), BF16),
            pltpu.VMEM((n_s, dec_rows, q_width), BF16),
            pltpu.VMEM((n_s, dec_rows, lanes), F32),
            pltpu.VMEM((q_width, width), BF16),
        ),
        in_specs=[anywhere] * 12,
        out_specs=(vmem, vmem, vmem, vmem),
        scratch_shapes=[
            pltpu.VMEM((rows, width), BF16),
            pltpu.VMEM(picks.shape, jnp.int32),
            pltpu.VMEM(gates.shape, F32),
            pltpu.VMEM(counts.shape, jnp.int32),
            pltpu.VMEM((1, width), F32),
            pltpu.VMEM((1, width), F32),
            pltpu.VMEM((width, hidden), BF16),
            pltpu.VMEM((hidden, width), BF16),
            pltpu.VMEM((width, q_width), BF16),
            pltpu.VMEM((width, q_width), BF16),
            pltpu.VMEM((n_s, dec_rows, q_width), BF16),
            pltpu.VMEM((n_e, slots, width), BF16),
            pltpu.VMEM((n_e, slots, width), BF16),
            pltpu.VMEM((n_e, slots, width), BF16),
            pltpu.VMEM((n_e, slots, width), BF16),
            pltpu.VMEM((n_s, dec_rows, q_width), BF16),
            pltpu.VMEM((n_s, dec_rows, lanes), F32),
            dma((12,)),
            dma((n_e,)),
            dma((n_e,)),
            dma((n_e,)),
            dma((n_e,)),
            dma((n_s,)),
            dma((n_s,)),
            dma((n_s,)),
            dma((n_s,)),
            dma((n_s,)),
            dma((n_s,)),
        ],
        compiler_params=pltpu.CompilerParams(
            collective_id=0, has_side_effects=True, vmem_limit_bytes=VMEM_BYTES - room
        ),
    )(
        tokens,
        picks,
        gates,
        counts,
        norm_in.reshape(1, -1),
        norm_out.reshape(1, -1),
        w_in,
        w_out,
        w_key,
        w_value,
        queries,
        w_proj,
    )
    return pl.pallas_call(
        finish,
        out_shape=(
            jax.ShapeDtypeStruct((rows, width), BF16),
            jax.ShapeDtypeStruct((dec_rows, width), BF16),
        ),
        in_specs=[vmem] * 4,
        out_specs=(anywhere, anywhere),
        scratch_shapes=[pltpu.VMEM((dec_rows, width), BF16), dma((2,))],
        compiler_params=pltpu.CompilerParams(vmem_limit_bytes=8 * 2**20),
    )(encoded, part, stat, w_proj_near)


def solution(mesh):
    in_specs = (
        P(("dp", "expert", "seq"), None),
        P(("dp", "expert", "seq"), None, None),
        P(("dp", "expert", "seq"), None, None),
        P(("dp", "expert", "seq"), None),
        P(),
        P(),
        P("expert", None, None),
        P("expert", None, None),
        P(),
        P(),
        P(("dp", "expert", "seq"), None),
        P(),
    )
    out_specs = (P(("dp", "expert", "seq"), None), P(("dp", "expert", "seq"), None))
    body = functools.partial(local, mesh.shape["expert"], mesh.shape["seq"])
    return jax.shard_map(body, mesh=mesh, in_specs=in_specs, out_specs=out_specs, check_vma=False)
```

```python
import functools

import jax
import jax.numpy as jnp
from jax import lax
from jax.experimental import pallas as pl
from jax.experimental.pallas import tpu as pltpu
from jax.sharding import PartitionSpec as P

HEADS = 8
EPSILON = 1e-06
VMEM_BYTES = 67043328
MESH = pl.DeviceIdType.MESH
GATHER_PIECES = 1
RETURN_PIECES = 1
F32 = jnp.float32
BF16 = jnp.bfloat16


def rms_norm(values, gain):
    mean_square = jnp.mean(values * values, axis=-1, keepdims=True)
    return values * lax.rsqrt(mean_square + EPSILON) * gain


def gelu(v):
    return 0.5 * v * (1.0 + jnp.tanh(0.7978845608028654 * (v + 0.044715 * v * v * v)))


def kernel(
    n_e,
    n_s,
    tokens_h,
    picks_h,
    gates_h,
    counts_h,
    norm_in_h,
    norm_out_h,
    w_in_h,
    w_out_h,
    w_key_h,
    w_value_h,
    queries_h,
    w_proj_h,
    enc_v,
    part_r,
    w_proj_v,
    tokens_v,
    picks_v,
    gates_v,
    counts_v,
    norm_in_v,
    norm_out_v,
    w_in_v,
    w_out_v,
    w_key_v,
    w_value_v,
    q_v,
    send_a,
    recv_a,
    send_b,
    recv_b,
    part_v,
    load_sem,
    a_send,
    a_recv,
    b_send,
    b_recv,
    q_send,
    q_recv,
    p_send,
    p_recv,
):
    me_e = lax.axis_index("expert")
    me_s = lax.axis_index("seq")
    upper = (2 * me_e) // n_e
    rows, width = tokens_v.shape
    slots = send_a.shape[1]
    dec_rows = q_v.shape[1]
    q_width = q_v.shape[2]
    head = q_width // HEADS

    loads = {}
    for i, (name, src, dst) in enumerate(
        (
            ("tokens", tokens_h, tokens_v),
            ("norm_in", norm_in_h, norm_in_v),
            ("picks", picks_h, picks_v),
            ("queries", queries_h, q_v.at[me_s]),
            ("w_in", w_in_h.at[0], w_in_v),
            ("w_out", w_out_h.at[0], w_out_v),
            ("gates", gates_h, gates_v),
            ("counts", counts_h, counts_v),
            ("norm_out", norm_out_h, norm_out_v),
            ("w_key", w_key_h, w_key_v),
            ("w_value", w_value_h, w_value_v),
            ("w_proj", w_proj_h, w_proj_v),
        )
    ):
        loads[name] = pltpu.make_async_copy(src, dst, load_sem.at[i])
        loads[name].start()

    barrier = pltpu.get_barrier_semaphore()
    for d in range(1, n_e):
        pl.semaphore_signal(
            barrier, inc=1, device_id={"expert": lax.rem(me_e + d, n_e)}, device_id_type=MESH
        )
    for d in range(1, n_s):
        pl.semaphore_signal(
            barrier, inc=1, device_id={"seq": lax.rem(me_s + d, n_s)}, device_id_type=MESH
        )

    loads["tokens"].wait()
    loads["norm_in"].wait()
    loads["picks"].wait()
    normed = rms_norm(tokens_v[...].astype(F32), norm_in_v[...]).astype(BF16)
    pick_row = jnp.concatenate([picks_v[0, j : j + 1, :] for j in range(n_e)], axis=1)
    position = lax.broadcasted_iota(jnp.int32, (rows, n_e * slots), 0)
    chosen = jnp.where(position == pick_row, 1.0, 0.0).astype(BF16)
    a_copies = []
    piece = width // GATHER_PIECES
    for c in range(GATHER_PIECES):
        cols = slice(c * piece, (c + 1) * piece)
        outgoing = lax.dot_general(
            chosen, normed[:, cols], (((0,), (0,)), ((), ())), preferred_element_type=F32
        ).astype(BF16)
        send_a[:, :, cols] = outgoing.reshape(n_e, slots, piece)
        if c == 0:
            pl.semaphore_wait(barrier, n_e - 1 + n_s - 1)
        for d in range(1, n_e):
            off = d * upper + (n_e - d) * (1 - upper)
            to = lax.rem(me_e + off, n_e)
            copy = pltpu.make_async_remote_copy(
                src_ref=send_a.at[to, :, cols],
                dst_ref=recv_a.at[off, :, cols],
                send_sem=a_send.at[c, off],
                recv_sem=a_recv.at[c, off],
                device_id={"expert": to},
                device_id_type=MESH,
            )
            copy.start()
            a_copies.append(copy)
    loads["queries"].wait()
    q_copies = []
    for d in range(1, n_s):
        copy = pltpu.make_async_remote_copy(
            src_ref=q_v.at[me_s],
            dst_ref=q_v.at[me_s],
            send_sem=q_send.at[d],
            recv_sem=q_recv.at[d],
            device_id={"seq": lax.rem(me_s + d, n_s)},
            device_id_type=MESH,
        )
        copy.start()
        q_copies.append(copy)
    recv_a[0] = send_a[me_e]

    loads["gates"].wait()
    loads["counts"].wait()
    slot = lax.broadcasted_iota(jnp.int32, (1, slots), 1)
    gate_row = jnp.concatenate(
        [
            jnp.where(slot < counts_v[0:1, j : j + 1], gates_v[0, j : j + 1, :], 0.0)
            for j in range(n_e)
        ],
        axis=1,
    )
    high = gate_row.astype(BF16).astype(F32)
    middle = (gate_row - high).astype(BF16).astype(F32)
    low = gate_row - high - middle
    gate_three = jnp.concatenate([high, middle, low], axis=1)
    pick_three = jnp.concatenate([pick_row] * 3, axis=1)
    position_three = lax.broadcasted_iota(jnp.int32, (rows, 3 * n_e * slots), 0)
    combine = jnp.where(position_three == pick_three, gate_three, 0.0).astype(BF16)

    loads["w_in"].wait()
    for c in range(GATHER_PIECES):
        cols = slice(c * (width // GATHER_PIECES), (c + 1) * (width // GATHER_PIECES))
        for d in range(1, n_e):
            pltpu.make_async_remote_copy(
                src_ref=send_a.at[lax.rem(me_e + d, n_e), :, cols],
                dst_ref=recv_a.at[d, :, cols],
                send_sem=a_send.at[c, d],
                recv_sem=a_recv.at[c, d],
                device_id={"expert": lax.rem(me_e + d, n_e)},
                device_id_type=MESH,
            ).wait_recv()
    flat = recv_a[...].reshape(n_e * slots, width)
    hidden = gelu(jnp.dot(flat, w_in_v[...], preferred_element_type=F32)).astype(BF16)
    loads["w_out"].wait()
    b_copies = []
    piece = width // RETURN_PIECES
    for c in range(RETURN_PIECES):
        cols = slice(c * piece, (c + 1) * piece)
        result = jnp.dot(hidden, w_out_v[:, cols], preferred_element_type=F32).astype(BF16)
        send_b[:, :, cols] = result.reshape(n_e, slots, piece)
        for d in range(1, n_e):
            off = d * (1 - upper) + (n_e - d) * upper
            copy = pltpu.make_async_remote_copy(
                src_ref=send_b.at[off, :, cols],
                dst_ref=recv_b.at[me_e, :, cols],
                send_sem=b_send.at[c, off],
                recv_sem=b_recv.at[c, off],
                device_id={"expert": lax.rem(me_e + n_e - off, n_e)},
                device_id_type=MESH,
            )
            copy.start()
            b_copies.append(copy)
    recv_b[me_e] = send_b[0]

    loads["norm_out"].wait()
    loads["w_key"].wait()
    loads["w_value"].wait()
    for c in range(RETURN_PIECES):
        cols = slice(c * piece, (c + 1) * piece)
        for d in range(1, n_e):
            pltpu.make_async_remote_copy(
                src_ref=send_b.at[d, :, cols],
                dst_ref=recv_b.at[lax.rem(me_e + d, n_e), :, cols],
                send_sem=b_send.at[c, d],
                recv_sem=b_recv.at[c, d],
                device_id={"expert": lax.rem(me_e + n_e - d, n_e)},
                device_id_type=MESH,
            ).wait_recv()
    returned = recv_b[...].reshape(n_e * slots, width)
    expert_sum = jnp.dot(
        combine, jnp.concatenate([returned] * 3, axis=0), preferred_element_type=F32
    )
    mixed = tokens_v[...].astype(F32) + expert_sum
    encoded = rms_norm(mixed, norm_out_v[...]).astype(BF16)
    enc_v[...] = encoded
    keys = jnp.dot(encoded, w_key_v[...], preferred_element_type=F32).astype(BF16)
    values = jnp.dot(encoded, w_value_v[...], preferred_element_type=F32).astype(BF16)

    for d in range(1, n_s):
        pltpu.make_async_remote_copy(
            src_ref=q_v.at[me_s],
            dst_ref=q_v.at[lax.rem(me_s + n_s - d, n_s)],
            send_sem=q_send.at[d],
            recv_sem=q_recv.at[d],
            device_id={"seq": lax.rem(me_s + d, n_s)},
            device_id_type=MESH,
        ).wait_recv()
    all_rows = n_s * dec_rows
    queries = q_v[...].reshape(all_rows, q_width)
    slab = min(256, q_width)
    group = slab // head
    lane_head = lax.broadcasted_iota(jnp.int32, (1, slab), 1) // head
    lanes = part_v.shape[2] - q_width
    stat_lane = lax.broadcasted_iota(jnp.int32, (1, lanes), 1)
    stats = jnp.zeros((all_rows, lanes), F32)
    p_copies = []
    groups = q_width // slab
    for g in range(groups):
        cols = slice(g * slab, (g + 1) * slab)
        stacked = jnp.concatenate(
            [
                queries[:, cols] * jnp.where(lane_head == h, 1.0, 0.0).astype(BF16)
                for h in range(group)
            ],
            axis=0,
        )
        scores = lax.dot_general(
            stacked, keys[:, cols], (((1,), (1,)), ((), ())), preferred_element_type=F32
        ) * (head**-0.5)
        row_max = jnp.max(scores, axis=1, keepdims=True)
        weights = jnp.exp(scores - row_max)
        row_total = jnp.sum(weights, axis=1, keepdims=True)
        product = jnp.dot(weights.astype(BF16), values[:, cols], preferred_element_type=F32)
        joined = product[:all_rows]
        for h in range(group):
            span = slice(h * all_rows, (h + 1) * all_rows)
            if h:
                joined = jnp.where(lane_head == h, product[span], joined)
            at = g * group + h
            stats = jnp.where(stat_lane == at, row_max[span], stats)
            stats = jnp.where(stat_lane == HEADS + at, row_total[span], stats)
        part_v[:, :, cols] = joined.astype(BF16).reshape(n_s, dec_rows, slab)
        if g == groups - 1:
            high = stats.astype(BF16).astype(F32)
            middle = (stats - high).astype(BF16).astype(F32)
            low = stats - high - middle
            packed = high + pltpu.roll(middle, 2 * HEADS, 1) + pltpu.roll(low, 4 * HEADS, 1)
            part_v[:, :, q_width:] = packed.astype(BF16).reshape(n_s, dec_rows, lanes)
    for d in range(1, n_s):
        to = lax.rem(me_s + d, n_s)
        copy = pltpu.make_async_remote_copy(
            src_ref=part_v.at[to],
            dst_ref=part_r.at[d],
            send_sem=p_send.at[d],
            recv_sem=p_recv.at[d],
            device_id={"seq": to},
            device_id_type=MESH,
        )
        copy.start()
        p_copies.append(copy)
    part_r[0] = part_v[me_s]
    for copy in p_copies:
        copy.wait_recv()
    for copy in a_copies + b_copies + q_copies + p_copies:
        copy.wait_send()
    loads["w_proj"].wait()


def finish(
    enc_v, part_v, w_proj_v, encoded_h, dec_h, dec_v, store_sem
):
    enc_store = pltpu.make_async_copy(enc_v, encoded_h, store_sem.at[0])
    enc_store.start()
    n_s, dec_rows, _ = part_v.shape
    q_width = w_proj_v.shape[0]
    head = q_width // HEADS
    part = [part_v[d, :, :q_width].astype(F32) for d in range(n_s)]
    stat = []
    for d in range(n_s):
        packed = part_v[d, :, q_width:].astype(F32)
        lanes = packed.shape[1]
        stat.append(
            packed
            + pltpu.roll(packed, lanes - 2 * HEADS, 1)
            + pltpu.roll(packed, lanes - 4 * HEADS, 1)
        )
    top = functools.reduce(jnp.maximum, stat)
    factor = [jnp.exp(s - top)[:, :HEADS] for s in stat]
    total = sum(f * s[:, HEADS : 2 * HEADS] for f, s in zip(factor, stat))
    lane = lax.broadcasted_iota(jnp.int32, (1, q_width), 1) // head
    summed = jnp.zeros((dec_rows, q_width), F32)
    for f, p in zip(factor, part):
        scale = f / total
        spread = jnp.zeros((dec_rows, q_width), F32)
        for h in range(HEADS):
            spread = jnp.where(lane == h, scale[:, h : h + 1], spread)
        summed = summed + spread * p
    dec_v[...] = jnp.dot(
        summed.astype(BF16), w_proj_v[...], preferred_element_type=F32
    ).astype(BF16)
    dec_store = pltpu.make_async_copy(dec_v, dec_h, store_sem.at[1])
    dec_store.start()
    enc_store.wait()
    dec_store.wait()


def local(
    n_e,
    n_s,
    tokens,
    picks,
    gates,
    counts,
    norm_in,
    norm_out,
    w_in,
    w_out,
    w_key,
    w_value,
    queries,
    w_proj,
):
    rows, width = tokens.shape
    slots = picks.shape[2]
    hidden = w_in.shape[2]
    dec_rows, q_width = queries.shape
    lanes = 128 * pl.cdiv(6 * HEADS, 128)
    anywhere = pl.BlockSpec(memory_space=pl.ANY)
    dma = pltpu.SemaphoreType.DMA
    vmem = pl.BlockSpec(memory_space=pltpu.VMEM)
    room = 2 * (rows * width + n_s * dec_rows * (q_width + lanes) + q_width * width)
    encoded, part, w_proj_near = pl.pallas_call(
        functools.partial(kernel, n_e, n_s),
        out_shape=(
            pltpu.VMEM((rows, width), BF16),
            pltpu.VMEM((n_s, dec_rows, q_width + lanes), BF16),
            pltpu.VMEM((q_width, width), BF16),
        ),
        in_specs=[anywhere] * 12,
        out_specs=(vmem, vmem, vmem),
        scratch_shapes=[
            pltpu.VMEM((rows, width), BF16),
            pltpu.VMEM(picks.shape, jnp.int32),
            pltpu.VMEM(gates.shape, F32),
            pltpu.VMEM(counts.shape, jnp.int32),
            pltpu.VMEM((1, width), F32),
            pltpu.VMEM((1, width), F32),
            pltpu.VMEM((width, hidden), BF16),
            pltpu.VMEM((hidden, width), BF16),
            pltpu.VMEM((width, q_width), BF16),
            pltpu.VMEM((width, q_width), BF16),
            pltpu.VMEM((n_s, dec_rows, q_width), BF16),
            pltpu.VMEM((n_e, slots, width), BF16),
            pltpu.VMEM((n_e, slots, width), BF16),
            pltpu.VMEM((n_e, slots, width), BF16),
            pltpu.VMEM((n_e, slots, width), BF16),
            pltpu.VMEM((n_s, dec_rows, q_width + lanes), BF16),
            dma((12,)),
            dma((GATHER_PIECES, n_e)),
            dma((GATHER_PIECES, n_e)),
            dma((RETURN_PIECES, n_e)),
            dma((RETURN_PIECES, n_e)),
            dma((n_s,)),
            dma((n_s,)),
            dma((n_s,)),
            dma((n_s,)),
        ],
        compiler_params=pltpu.CompilerParams(
            collective_id=0, has_side_effects=True, vmem_limit_bytes=VMEM_BYTES - room
        ),
    )(
        tokens,
        picks,
        gates,
        counts,
        norm_in.reshape(1, -1),
        norm_out.reshape(1, -1),
        w_in,
        w_out,
        w_key,
        w_value,
        queries,
        w_proj,
    )
    return pl.pallas_call(
        finish,
        out_shape=(
            jax.ShapeDtypeStruct((rows, width), BF16),
            jax.ShapeDtypeStruct((dec_rows, width), BF16),
        ),
        in_specs=[vmem] * 3,
        out_specs=(anywhere, anywhere),
        scratch_shapes=[pltpu.VMEM((dec_rows, width), BF16), dma((2,))],
        compiler_params=pltpu.CompilerParams(vmem_limit_bytes=8 * 2**20),
    )(encoded, part, w_proj_near)


def solution(mesh):
    in_specs = (
        P(("dp", "expert", "seq"), None),
        P(("dp", "expert", "seq"), None, None),
        P(("dp", "expert", "seq"), None, None),
        P(("dp", "expert", "seq"), None),
        P(),
        P(),
        P("expert", None, None),
        P("expert", None, None),
        P(),
        P(),
        P(("dp", "expert", "seq"), None),
        P(),
    )
    out_specs = (P(("dp", "expert", "seq"), None), P(("dp", "expert", "seq"), None))
    body = functools.partial(local, mesh.shape["expert"], mesh.shape["seq"])
    return jax.shard_map(body, mesh=mesh, in_specs=in_specs, out_specs=out_specs, check_vma=False)
```

```python
import functools

import jax
import jax.numpy as jnp
from jax import lax
from jax.experimental import pallas as pl
from jax.experimental.pallas import tpu as pltpu
from jax.sharding import PartitionSpec as P

HEADS = 8
EPSILON = 1e-06
VMEM_BYTES = 67043328
MESH = pl.DeviceIdType.MESH
GATHER_PIECES = 1
RETURN_PIECES = 1
F32 = jnp.float32
BF16 = jnp.bfloat16


def rms_norm(values, gain):
    mean_square = jnp.mean(values * values, axis=-1, keepdims=True)
    return values * lax.rsqrt(mean_square + EPSILON) * gain


def gelu(v):
    return 0.5 * v * (1.0 + jnp.tanh(0.7978845608028654 * (v + 0.044715 * v * v * v)))


def kernel(
    n_e,
    n_s,
    tokens_h,
    picks_h,
    gates_h,
    counts_h,
    norm_in_h,
    norm_out_h,
    w_in_h,
    w_out_h,
    w_key_h,
    w_value_h,
    queries_h,
    w_proj_h,
    enc_v,
    part_r,
    w_proj_v,
    tokens_v,
    picks_v,
    gates_v,
    counts_v,
    norm_in_v,
    norm_out_v,
    w_in_v,
    w_out_v,
    w_key_v,
    w_value_v,
    q_v,
    send_a,
    recv_a,
    send_b,
    recv_b,
    part_v,
    load_sem,
    a_send,
    a_recv,
    b_send,
    b_recv,
    q_send,
    q_recv,
    p_send,
    p_recv,
):
    me_e = lax.axis_index("expert")
    me_s = lax.axis_index("seq")
    upper = (2 * me_e) // n_e
    rows, width = tokens_v.shape
    slots = send_a.shape[1]
    dec_rows = q_v.shape[1]
    q_width = q_v.shape[2]
    head = q_width // HEADS

    barrier = pltpu.get_barrier_semaphore()
    for d in range(1, n_e):
        pl.semaphore_signal(
            barrier, inc=1, device_id={"expert": lax.rem(me_e + d, n_e)}, device_id_type=MESH
        )
    for d in range(1, n_s):
        pl.semaphore_signal(
            barrier, inc=1, device_id={"seq": lax.rem(me_s + d, n_s)}, device_id_type=MESH
        )

    loads = {}
    for i, (name, src, dst) in enumerate(
        (
            ("tokens", tokens_h, tokens_v),
            ("norm_in", norm_in_h, norm_in_v),
            ("picks", picks_h, picks_v),
            ("queries", queries_h, q_v.at[me_s]),
            ("w_in", w_in_h.at[0], w_in_v),
            ("w_out", w_out_h.at[0], w_out_v),
            ("gates", gates_h, gates_v),
            ("counts", counts_h, counts_v),
            ("norm_out", norm_out_h, norm_out_v),
            ("w_key", w_key_h, w_key_v),
            ("w_value", w_value_h, w_value_v),
            ("w_proj", w_proj_h, w_proj_v),
        )
    ):
        loads[name] = pltpu.make_async_copy(src, dst, load_sem.at[i])
        loads[name].start()

    loads["tokens"].wait()
    loads["norm_in"].wait()
    loads["picks"].wait()
    normed = rms_norm(tokens_v[...].astype(F32), norm_in_v[...]).astype(BF16)
    pick_row = jnp.concatenate([picks_v[0, j : j + 1, :] for j in range(n_e)], axis=1)
    position = lax.broadcasted_iota(jnp.int32, (rows, n_e * slots), 0)
    chosen = jnp.where(position == pick_row, 1.0, 0.0).astype(BF16)
    a_copies = []
    piece = width // GATHER_PIECES
    for c in range(GATHER_PIECES):
        cols = slice(c * piece, (c + 1) * piece)
        outgoing = lax.dot_general(
            chosen, normed[:, cols], (((0,), (0,)), ((), ())), preferred_element_type=F32
        ).astype(BF16)
        send_a[:, :, cols] = outgoing.reshape(n_e, slots, piece)
        if c == 0:
            pl.semaphore_wait(barrier, n_e - 1 + n_s - 1)
        for d in range(1, n_e):
            off = d * upper + (n_e - d) * (1 - upper)
            to = lax.rem(me_e + off, n_e)
            copy = pltpu.make_async_remote_copy(
                src_ref=send_a.at[to, :, cols],
                dst_ref=recv_a.at[off, :, cols],
                send_sem=a_send.at[c, off],
                recv_sem=a_recv.at[c, off],
                device_id={"expert": to},
                device_id_type=MESH,
            )
            copy.start()
            a_copies.append(copy)
    loads["queries"].wait()
    q_copies = []
    for d in range(1, n_s):
        copy = pltpu.make_async_remote_copy(
            src_ref=q_v.at[me_s],
            dst_ref=q_v.at[me_s],
            send_sem=q_send.at[d],
            recv_sem=q_recv.at[d],
            device_id={"seq": lax.rem(me_s + d, n_s)},
            device_id_type=MESH,
        )
        copy.start()
        q_copies.append(copy)
    recv_a[0] = send_a[me_e]

    loads["gates"].wait()
    loads["counts"].wait()
    slot = lax.broadcasted_iota(jnp.int32, (1, slots), 1)
    gate_row = jnp.concatenate(
        [
            jnp.where(slot < counts_v[0:1, j : j + 1], gates_v[0, j : j + 1, :], 0.0)
            for j in range(n_e)
        ],
        axis=1,
    )
    high = gate_row.astype(BF16).astype(F32)
    middle = (gate_row - high).astype(BF16).astype(F32)
    low = gate_row - high - middle
    gate_three = jnp.concatenate([high, middle, low], axis=1)
    pick_three = jnp.concatenate([pick_row] * 3, axis=1)
    position_three = lax.broadcasted_iota(jnp.int32, (rows, 3 * n_e * slots), 0)
    combine = jnp.where(position_three == pick_three, gate_three, 0.0).astype(BF16)

    loads["w_in"].wait()
    for c in range(GATHER_PIECES):
        cols = slice(c * (width // GATHER_PIECES), (c + 1) * (width // GATHER_PIECES))
        for d in range(1, n_e):
            pltpu.make_async_remote_copy(
                src_ref=send_a.at[lax.rem(me_e + d, n_e), :, cols],
                dst_ref=recv_a.at[d, :, cols],
                send_sem=a_send.at[c, d],
                recv_sem=a_recv.at[c, d],
                device_id={"expert": lax.rem(me_e + d, n_e)},
                device_id_type=MESH,
            ).wait_recv()
    flat = recv_a[...].reshape(n_e * slots, width)
    hidden = gelu(jnp.dot(flat, w_in_v[...], preferred_element_type=F32)).astype(BF16)
    loads["w_out"].wait()
    b_copies = []
    piece = width // RETURN_PIECES
    for c in range(RETURN_PIECES):
        cols = slice(c * piece, (c + 1) * piece)
        result = jnp.dot(hidden, w_out_v[:, cols], preferred_element_type=F32).astype(BF16)
        send_b[:, :, cols] = result.reshape(n_e, slots, piece)
        for d in range(1, n_e):
            off = d * (1 - upper) + (n_e - d) * upper
            copy = pltpu.make_async_remote_copy(
                src_ref=send_b.at[off, :, cols],
                dst_ref=recv_b.at[me_e, :, cols],
                send_sem=b_send.at[c, off],
                recv_sem=b_recv.at[c, off],
                device_id={"expert": lax.rem(me_e + n_e - off, n_e)},
                device_id_type=MESH,
            )
            copy.start()
            b_copies.append(copy)
    recv_b[me_e] = send_b[0]

    loads["norm_out"].wait()
    loads["w_key"].wait()
    loads["w_value"].wait()
    for c in range(RETURN_PIECES):
        cols = slice(c * piece, (c + 1) * piece)
        for d in range(1, n_e):
            pltpu.make_async_remote_copy(
                src_ref=send_b.at[d, :, cols],
                dst_ref=recv_b.at[lax.rem(me_e + d, n_e), :, cols],
                send_sem=b_send.at[c, d],
                recv_sem=b_recv.at[c, d],
                device_id={"expert": lax.rem(me_e + n_e - d, n_e)},
                device_id_type=MESH,
            ).wait_recv()
    returned = recv_b[...].reshape(n_e * slots, width)
    expert_sum = jnp.dot(
        combine, jnp.concatenate([returned] * 3, axis=0), preferred_element_type=F32
    )
    mixed = tokens_v[...].astype(F32) + expert_sum
    encoded = rms_norm(mixed, norm_out_v[...]).astype(BF16)
    enc_v[...] = encoded
    keys = jnp.dot(encoded, w_key_v[...], preferred_element_type=F32).astype(BF16)
    values = jnp.dot(encoded, w_value_v[...], preferred_element_type=F32).astype(BF16)

    for d in range(1, n_s):
        pltpu.make_async_remote_copy(
            src_ref=q_v.at[me_s],
            dst_ref=q_v.at[lax.rem(me_s + n_s - d, n_s)],
            send_sem=q_send.at[d],
            recv_sem=q_recv.at[d],
            device_id={"seq": lax.rem(me_s + d, n_s)},
            device_id_type=MESH,
        ).wait_recv()
    all_rows = n_s * dec_rows
    queries = q_v[...].reshape(all_rows, q_width)
    slab = min(256, q_width)
    group = slab // head
    lane_head = lax.broadcasted_iota(jnp.int32, (1, slab), 1) // head
    lanes = part_v.shape[2] - q_width
    stat_lane = lax.broadcasted_iota(jnp.int32, (1, lanes), 1)
    stats = jnp.zeros((all_rows, lanes), F32)
    p_copies = []
    groups = q_width // slab
    for g in range(groups):
        cols = slice(g * slab, (g + 1) * slab)
        stacked = jnp.concatenate(
            [
                queries[:, cols] * jnp.where(lane_head == h, 1.0, 0.0).astype(BF16)
                for h in range(group)
            ],
            axis=0,
        )
        scores = lax.dot_general(
            stacked, keys[:, cols], (((1,), (1,)), ((), ())), preferred_element_type=F32
        ) * (head**-0.5)
        row_max = jnp.max(scores, axis=1, keepdims=True)
        weights = jnp.exp(scores - row_max)
        row_total = jnp.sum(weights, axis=1, keepdims=True)
        product = jnp.dot(weights.astype(BF16), values[:, cols], preferred_element_type=F32)
        joined = product[:all_rows]
        for h in range(group):
            span = slice(h * all_rows, (h + 1) * all_rows)
            if h:
                joined = jnp.where(lane_head == h, product[span], joined)
            at = g * group + h
            stats = jnp.where(stat_lane == at, row_max[span], stats)
            stats = jnp.where(stat_lane == HEADS + at, row_total[span], stats)
        part_v[:, :, cols] = joined.astype(BF16).reshape(n_s, dec_rows, slab)
        if g == groups - 1:
            high = stats.astype(BF16).astype(F32)
            middle = (stats - high).astype(BF16).astype(F32)
            low = stats - high - middle
            packed = high + pltpu.roll(middle, 2 * HEADS, 1) + pltpu.roll(low, 4 * HEADS, 1)
            part_v[:, :, q_width:] = packed.astype(BF16).reshape(n_s, dec_rows, lanes)
    for d in range(1, n_s):
        to = lax.rem(me_s + d, n_s)
        copy = pltpu.make_async_remote_copy(
            src_ref=part_v.at[to],
            dst_ref=part_r.at[d],
            send_sem=p_send.at[d],
            recv_sem=p_recv.at[d],
            device_id={"seq": to},
            device_id_type=MESH,
        )
        copy.start()
        p_copies.append(copy)
    part_r[0] = part_v[me_s]
    for copy in p_copies:
        copy.wait_recv()
    for copy in a_copies + b_copies + q_copies + p_copies:
        copy.wait_send()
    loads["w_proj"].wait()


def finish(
    enc_v, part_v, w_proj_v, encoded_h, dec_h, dec_v, store_sem
):
    enc_store = pltpu.make_async_copy(enc_v, encoded_h, store_sem.at[0])
    enc_store.start()
    n_s, dec_rows, _ = part_v.shape
    q_width = w_proj_v.shape[0]
    head = q_width // HEADS
    part = [part_v[d, :, :q_width].astype(F32) for d in range(n_s)]
    stat = []
    for d in range(n_s):
        packed = part_v[d, :, q_width:].astype(F32)
        lanes = packed.shape[1]
        stat.append(
            packed
            + pltpu.roll(packed, lanes - 2 * HEADS, 1)
            + pltpu.roll(packed, lanes - 4 * HEADS, 1)
        )
    top = functools.reduce(jnp.maximum, stat)
    factor = [jnp.exp(s - top)[:, :HEADS] for s in stat]
    total = sum(f * s[:, HEADS : 2 * HEADS] for f, s in zip(factor, stat))
    lane = lax.broadcasted_iota(jnp.int32, (1, q_width), 1) // head
    summed = jnp.zeros((dec_rows, q_width), F32)
    for f, p in zip(factor, part):
        scale = f / total
        spread = jnp.zeros((dec_rows, q_width), F32)
        for h in range(HEADS):
            spread = jnp.where(lane == h, scale[:, h : h + 1], spread)
        summed = summed + spread * p
    dec_v[...] = jnp.dot(
        summed.astype(BF16), w_proj_v[...], preferred_element_type=F32
    ).astype(BF16)
    dec_store = pltpu.make_async_copy(dec_v, dec_h, store_sem.at[1])
    dec_store.start()
    enc_store.wait()
    dec_store.wait()


def local(
    n_e,
    n_s,
    tokens,
    picks,
    gates,
    counts,
    norm_in,
    norm_out,
    w_in,
    w_out,
    w_key,
    w_value,
    queries,
    w_proj,
):
    rows, width = tokens.shape
    slots = picks.shape[2]
    hidden = w_in.shape[2]
    dec_rows, q_width = queries.shape
    lanes = 128 * pl.cdiv(6 * HEADS, 128)
    anywhere = pl.BlockSpec(memory_space=pl.ANY)
    dma = pltpu.SemaphoreType.DMA
    vmem = pl.BlockSpec(memory_space=pltpu.VMEM)
    room = 2 * (rows * width + n_s * dec_rows * (q_width + lanes) + q_width * width)
    encoded, part, w_proj_near = pl.pallas_call(
        functools.partial(kernel, n_e, n_s),
        out_shape=(
            pltpu.VMEM((rows, width), BF16),
            pltpu.VMEM((n_s, dec_rows, q_width + lanes), BF16),
            pltpu.VMEM((q_width, width), BF16),
        ),
        in_specs=[anywhere] * 12,
        out_specs=(vmem, vmem, vmem),
        scratch_shapes=[
            pltpu.VMEM((rows, width), BF16),
            pltpu.VMEM(picks.shape, jnp.int32),
            pltpu.VMEM(gates.shape, F32),
            pltpu.VMEM(counts.shape, jnp.int32),
            pltpu.VMEM((1, width), F32),
            pltpu.VMEM((1, width), F32),
            pltpu.VMEM((width, hidden), BF16),
            pltpu.VMEM((hidden, width), BF16),
            pltpu.VMEM((width, q_width), BF16),
            pltpu.VMEM((width, q_width), BF16),
            pltpu.VMEM((n_s, dec_rows, q_width), BF16),
            pltpu.VMEM((n_e, slots, width), BF16),
            pltpu.VMEM((n_e, slots, width), BF16),
            pltpu.VMEM((n_e, slots, width), BF16),
            pltpu.VMEM((n_e, slots, width), BF16),
            pltpu.VMEM((n_s, dec_rows, q_width + lanes), BF16),
            dma((12,)),
            dma((GATHER_PIECES, n_e)),
            dma((GATHER_PIECES, n_e)),
            dma((RETURN_PIECES, n_e)),
            dma((RETURN_PIECES, n_e)),
            dma((n_s,)),
            dma((n_s,)),
            dma((n_s,)),
            dma((n_s,)),
        ],
        compiler_params=pltpu.CompilerParams(
            collective_id=0, has_side_effects=True, vmem_limit_bytes=VMEM_BYTES - room
        ),
    )(
        tokens,
        picks,
        gates,
        counts,
        norm_in.reshape(1, -1),
        norm_out.reshape(1, -1),
        w_in,
        w_out,
        w_key,
        w_value,
        queries,
        w_proj,
    )
    return pl.pallas_call(
        finish,
        out_shape=(
            jax.ShapeDtypeStruct((rows, width), BF16),
            jax.ShapeDtypeStruct((dec_rows, width), BF16),
        ),
        in_specs=[vmem] * 3,
        out_specs=(anywhere, anywhere),
        scratch_shapes=[pltpu.VMEM((dec_rows, width), BF16), dma((2,))],
        compiler_params=pltpu.CompilerParams(vmem_limit_bytes=8 * 2**20),
    )(encoded, part, w_proj_near)


def solution(mesh):
    in_specs = (
        P(("dp", "expert", "seq"), None),
        P(("dp", "expert", "seq"), None, None),
        P(("dp", "expert", "seq"), None, None),
        P(("dp", "expert", "seq"), None),
        P(),
        P(),
        P("expert", None, None),
        P("expert", None, None),
        P(),
        P(),
        P(("dp", "expert", "seq"), None),
        P(),
    )
    out_specs = (P(("dp", "expert", "seq"), None), P(("dp", "expert", "seq"), None))
    body = functools.partial(local, mesh.shape["expert"], mesh.shape["seq"])
    return jax.shard_map(body, mesh=mesh, in_specs=in_specs, out_specs=out_specs, check_vma=False)
```
